32 devices in a mesh: ep: 8 (over y, x, core), dp: 4 (over z).
Axes of the slice: x: 2, y: 2, z: 4, core: 2. Of those that a mesh axis runs over, the one named last changes fastest.
Arguments:
- tokens: bfloat16 [64, 7168], P('dp', 'ep'), may hold values from -6 to 6
- norm_gain: float32 [2, 7168], replicated, may hold values from 0.1 to 1.9
- gate_weight: bfloat16 [2, 12, 2048, 7168], P(None, 'dp', 'ep'), may hold values from -0.0625 to 0.0625
- up_weight: bfloat16 [2, 12, 2048, 7168], P(None, 'dp', 'ep'), may hold values from -0.0625 to 0.0625
- down_weight: bfloat16 [2, 12, 7168, 2048], P(None, 'dp', 'ep'), may hold values from -0.125 to 0.125
- replica_plan: int32 [2, 4, 2], replicated, may hold values from 0 to 2
- route_expert: int32 [2, 64, 8], replicated, may hold values from 0 to 11, as said below
- replica_pick: int32 [2, 64, 8], replicated, may hold values from 0 to 2
- combine_num: int32 [2, 64, 8], P(None, 'dp'), may hold values from 1 to 8
Outputs:
- stream_out: bfloat16 [64, 7168], P('dp', 'ep')
- last_update: bfloat16 [64, 7168], P('dp', 'ep')
The draws below stay inside these ranges and needn't reach their ends.
Inputs may be any that keep to these rules, and one draw needn't show every extreme that they name: `route_expert`: each row of one layer names 8 different experts.
All inputs are finite; a program needn't handle non-finite values.
Results may differ from the reference program's by a relative error of at most 0.011.
Values may be sent and summed in bfloat16 or wider, within the bound.
No kernel may reach another device: no remote copies, remote signals or barrier semaphores. Data moves between devices by JAX's collectives and lax.ppermute only.
A program may use at most 256 MiB of HBM per device.

```python
import jax
import jax.numpy as jnp
from jax import lax

D = 7168
FF = 2048
TOPK = 8
EXP_HOST = 3
REP_HOST = 2
LAYERS = 2
TOK_GRP = 16
CAP = 8
EXPERTS = 12
TOKENS = 64
N_DP = 4


def hot_choice(key):
    return jax.random.randint(jax.random.fold_in(key, 7), (LAYERS, TOKENS // TOK_GRP), 0, EXPERTS).astype(jnp.int32)


def hot_rows(key):
    hot = hot_choice(key)
    group_of = jnp.arange(TOKENS, dtype=jnp.int32) // TOK_GRP
    return hot[:, group_of]


def draw_route_expert(key, part):
    noise = jax.random.randint(jax.random.fold_in(key, 11), (LAYERS, TOKENS, EXPERTS), 0, 2 ** 18)
    favour = jax.random.randint(jax.random.fold_in(key, 13), (LAYERS, 1, EXPERTS), 0, 3) * 2 ** 18
    column = jnp.arange(EXPERTS, dtype=jnp.int32)
    boost = (column[None, None, :] == hot_rows(key)[:, :, None]).astype(jnp.int32) * 2 ** 22
    scores = (noise + favour + boost) * EXPERTS + column[None, None, :]
    values, picked = lax.top_k(scores, TOPK)
    return picked.astype(jnp.int32)


def draw_replica_pick(key, part):
    routes = draw_route_expert(key, part)
    picks = jax.random.randint(jax.random.fold_in(key, 17), (LAYERS, TOKENS, TOPK), 0, 3)
    return jnp.where(routes == hot_rows(key)[:, :, None], 0, picks).astype(jnp.int32)


def set_ends(entries, rng, low, top_value):
    longest = entries.shape.index(max(entries.shape))
    spots = []
    for shift in (0, 1):
        where = [jax.random.randint(jax.random.fold_in(rng, axis), (), 0, length) for axis, length in enumerate(entries.shape)]
        where[longest] = (where[longest] + shift) % entries.shape[longest]
        spots.append(tuple(where))
    return entries.at[spots[0]].set(low).at[spots[1]].set(top_value)


def steps_of(own_key, extent, shards, low, largest):
    factor_of = 1.0
    for dim, parts in shards:
        steps = jax.random.uniform(jax.random.fold_in(jax.random.fold_in(own_key, 6), dim), (parts,), jnp.float32, low / len(shards), largest / len(shards))
        factor_of = factor_of * jnp.repeat(jnp.exp(steps), extent[dim] // parts).reshape((-1,) + (1,) * (len(extent) - 1 - dim))
    return factor_of


def gaussian(stream_key, shape, deviation, most, shards=(), kind=jnp.bfloat16):
    values = deviation * jax.random.normal(stream_key, shape, jnp.float32)
    if shards:
        values = values * steps_of(stream_key, shape, shards, -0.22, 0.18)
    return jnp.clip(values, -most, most).astype(kind)


def setup_inputs(seed: int = 0) -> dict:
    key_list = jax.random.split(jax.random.key(seed), 10)
    tokens = gaussian(key_list[0], (TOKENS, D), 1.0, 6.0, ((0, 4), (1, 8)))
    norm_gain = jnp.clip(1.0 + 0.18 * jax.random.normal(key_list[1], (LAYERS, D), jnp.float32), 0.1, 1.9)
    gate_weight = gaussian(key_list[2], (LAYERS, EXPERTS, FF, D), D ** -0.5, 0.0625, ((1, 4), (2, 8)))
    up_weight = gaussian(key_list[3], (LAYERS, EXPERTS, FF, D), D ** -0.5, 0.0625, ((1, 4), (2, 8)))
    down_weight = gaussian(key_list[4], (LAYERS, EXPERTS, D, FF), FF ** -0.5, 0.125, ((1, 4), (2, 8)))
    replica_plan = set_ends(jax.random.randint(key_list[5], (LAYERS, N_DP, REP_HOST), 0, EXP_HOST), jax.random.fold_in(key_list[5], 1), 0, EXP_HOST - 1).astype(jnp.int32)
    route_expert = draw_route_expert(jax.random.fold_in(key_list[9], 71), 0)
    replica_pick = draw_replica_pick(jax.random.fold_in(key_list[9], 71), 0)
    combine_num = set_ends(jax.random.randint(key_list[8], (LAYERS, TOKENS, TOPK), 1, 9), jax.random.fold_in(key_list[8], 1), 1, 8).astype(jnp.int32)
    return dict(tokens=tokens, norm_gain=norm_gain, gate_weight=gate_weight, up_weight=up_weight, down_weight=down_weight, replica_plan=replica_plan, route_expert=route_expert, replica_pick=replica_pick, combine_num=combine_num)


epsilon = 1e-06

def serve_table(plan_layer):
    replicas = EXP_HOST + REP_HOST
    flat_ids = jnp.arange(N_DP * replicas, dtype=jnp.int32)
    host_of = flat_ids // replicas
    local_id = flat_ids % replicas
    copy_id = jnp.clip(local_id - EXP_HOST, 0, REP_HOST - 1)
    owner = (host_of - 1 - copy_id) % N_DP
    copied = owner * EXP_HOST + plan_layer[host_of, copy_id]
    return jnp.where(local_id < EXP_HOST, host_of * EXP_HOST + local_id, copied).astype(jnp.int32)

def targets(experts_g, picks_g, table):
    flat_e = experts_g.reshape(-1)
    flat_p = picks_g.reshape(-1)
    matches = (table[None, :] == flat_e[:, None]).astype(jnp.int32)
    counts = lax.optimization_barrier(jnp.sum(matches, axis=1))
    rank_in = jnp.cumsum(matches, axis=1) - 1
    wanted = flat_p % counts
    chosen = matches * (rank_in == wanted[:, None]).astype(jnp.int32)
    target = lax.optimization_barrier(jnp.sum(chosen * jnp.arange(table.shape[0], dtype=jnp.int32)[None, :], axis=1))
    before = jnp.cumsum(chosen, axis=0) - chosen
    position = lax.optimization_barrier(jnp.sum(before * chosen, axis=1))
    return (target.astype(jnp.int32), position.astype(jnp.int32))

def reference(tokens, norm_gain, gate_weight, up_weight, down_weight, replica_plan, route_expert, replica_pick, combine_num):
    stream = tokens
    update = jnp.zeros((TOKENS, D), jnp.float32)
    for layer_id in range(LAYERS):
        stream_f = stream.astype(jnp.float32)
        mean_sq = lax.optimization_barrier(jnp.mean(stream_f * stream_f, axis=1, keepdims=True))
        normed = (stream_f * lax.rsqrt(mean_sq + epsilon) * norm_gain[layer_id][None, :]).astype(jnp.bfloat16)

        def one_expert(weights):
            gate_act = jnp.dot(normed, weights[0].T, preferred_element_type=jnp.float32)
            up_act = jnp.dot(normed, weights[1].T, preferred_element_type=jnp.float32)
            hidden = (jax.nn.silu(gate_act) * up_act).astype(jnp.bfloat16)
            return jnp.dot(hidden, weights[2].T, preferred_element_type=jnp.float32).astype(jnp.bfloat16)
        every_out = lax.map(one_expert, (gate_weight[layer_id], up_weight[layer_id], down_weight[layer_id]))
        table = serve_table(replica_plan[layer_id])
        experts_l = route_expert[layer_id]
        grouped_e = experts_l.reshape(N_DP, TOK_GRP, TOPK)
        grouped_p = replica_pick[layer_id].reshape(N_DP, TOK_GRP, TOPK)
        target, position = jax.vmap(lambda e_blk, p_blk: targets(e_blk, p_blk, table))(grouped_e, grouped_p)
        kept_mask = (position.reshape(TOKENS, TOPK) < CAP).astype(jnp.float32)
        flat_e = experts_l.reshape(-1)
        token_ids = jnp.repeat(jnp.arange(TOKENS, dtype=jnp.int32), TOPK)
        picked = every_out[flat_e, token_ids].astype(jnp.float32).reshape(TOKENS, TOPK, D)
        numerator = combine_num[layer_id].astype(jnp.float32)
        weights_k = numerator / lax.optimization_barrier(jnp.sum(numerator, axis=1, keepdims=True))
        combine = weights_k * kept_mask
        update = lax.optimization_barrier(jnp.sum(combine[:, :, None] * picked, axis=1))
        stream = (stream.astype(jnp.float32) + update).astype(jnp.bfloat16)
    return (stream, update.astype(jnp.bfloat16))
```

```python
import functools

import jax
import jax.numpy as jnp
from jax import lax
from jax.experimental import pallas as pl
from jax.experimental.pallas import tpu as pltpu
from jax.sharding import PartitionSpec as P


epsilon = 1e-06
lanes = 128
bf16 = jnp.bfloat16
f32 = jnp.float32


def routing_kernel(plan_ref, route_ref, pick_ref, mask_ref, *, sizes):
    layers, groups, rows, top, exp_host, rep_host, capacity = sizes
    host = lax.axis_index("dp")
    replicas = exp_host + rep_host
    tokens = groups * rows
    slots = -(-groups * replicas // 8) * 8
    slot_i = lax.broadcasted_iota(jnp.int32, (slots, 1), 0)
    from_i = lax.broadcasted_iota(jnp.int32, (tokens, lanes), 0)
    to_i = lax.broadcasted_iota(jnp.int32, (tokens, lanes), 1)
    earlier = jnp.where((from_i // rows == to_i // rows) & (from_i < to_i), 1.0, 0.0).astype(bf16)[:, :tokens]
    swap = jnp.where((from_i // rows == (to_i // rows) ^ host) & (from_i % rows == to_i % rows), 1.0, 0.0).astype(bf16)
    for layer in range(layers):
        served = []
        for slot in range(groups * replicas):
            owner, local = divmod(slot, replicas)
            if local < exp_host:
                served.append(owner * exp_host + local)
            else:
                copy = local - exp_host
                served.append(((owner - 1 - copy) % groups) * exp_host + plan_ref[layer, copy, owner])
        table = jnp.full((slots, 1), -1, jnp.int32)
        for slot, expert in enumerate(served):
            table = jnp.where(slot_i == slot, expert, table)
        rank = jnp.zeros((slots, 1), f32)
        count = jnp.zeros((slots, 1), f32)
        for slot, expert in enumerate(served):
            same = jnp.where(table == expert, 1.0, 0.0)
            count = count + same
            rank = rank + jnp.where(slot_i > slot, same, 0.0)
        count = jnp.broadcast_to(jnp.maximum(count, 1.0), (slots, tokens))
        rank = jnp.broadcast_to(rank, (slots, tokens))
        table = jnp.broadcast_to(table, (slots, tokens))
        experts = route_ref[layer]
        picks = pick_ref[layer].astype(f32)
        chosen = []
        for k in range(top):
            pick = picks[k : k + 1, :]
            wanted = pick - count * jnp.floor((pick + 0.5) / count)
            chosen.append(jnp.where((experts[k : k + 1, :] == table) & (rank == wanted), 1.0, 0.0))
        total = functools.reduce(lambda a, b: a + b, chosen)
        before = jnp.dot(total.astype(bf16), earlier, preferred_element_type=f32)
        kept = []
        for k in range(top):
            position = jnp.sum(before * chosen[k], axis=0, keepdims=True)
            before = before + chosen[k]
            kept.append(jnp.where(position < capacity - 0.5, 1.0, 0.0))
        kept = jnp.concatenate(kept, axis=0)
        for j in range(exp_host):
            mask = jnp.where(experts == host * exp_host + j, kept, 0.0)
            mask_ref[layer, j] = jnp.dot(mask.astype(bf16), swap, preferred_element_type=f32)


def gate_kernel(mask_ref, num_ref, gain_ref, *refs, layer, top, rows, shards, exp_host, units, width):
    x_refs = refs[:shards]
    gate_hbm, up_hbm, out_ref, gate_buf, up_buf, acc_ref, sems = refs[shards:]
    column = lax.axis_index("ep")
    pairs = shards // 2
    pair_width = 2 * width
    full = shards * width

    def copies(m):
        offset = pl.multiple_of(((column // 2) ^ m) * pair_width, lanes)
        return [
            pltpu.make_async_copy(src.at[layer, :, :, pl.ds(offset, pair_width)], dst.at[m], sems.at[i, m])
            for i, (src, dst) in enumerate(((gate_hbm, gate_buf), (up_hbm, up_buf)))
        ]

    for m in range(pairs):
        for c in copies(m):
            c.start()
    tokens = x_refs[0].shape[0]
    odd = column % 2 == 1
    squares = jnp.zeros((tokens, 1), f32)
    for m in range(pairs):
        mine = x_refs[2 * m][...].astype(f32)
        other = x_refs[2 * m + 1][...].astype(f32)
        squares = squares + jnp.sum(mine * mine + other * other, axis=1, keepdims=True)
        both = jnp.concatenate([jnp.where(odd, other, mine), jnp.where(odd, mine, other)], axis=1)
        offset = pl.multiple_of(((column // 2) ^ m) * pair_width, lanes)
        gain = gain_ref[layer : layer + 1, pl.ds(offset, pair_width)]
        scaled = (both * gain).astype(bf16)
        waits = copies(m)
        for i, buf in enumerate((gate_buf, up_buf)):
            waits[i].wait()
            part = lax.dot_general(
                buf[m].reshape(exp_host * units, pair_width),
                scaled,
                (((1,), (1,)), ((), ())),
                preferred_element_type=f32,
            )
            if m == 0:
                acc_ref[i, :, :tokens] = part
            else:
                acc_ref[i, :, :tokens] = acc_ref[i, :, :tokens] + part
    inverse = lax.rsqrt(squares / full + epsilon)
    turned = jnp.concatenate([jnp.broadcast_to(inverse, (tokens, lanes)), jnp.zeros((lanes - tokens, lanes), f32)], axis=0).T
    scale = turned[0:1, :]
    blocks = num_ref.shape[0] // rows
    numbers = num_ref[0:rows, :].astype(f32)
    for b in range(1, blocks):
        numbers = numbers + pltpu.roll(num_ref[b * rows : (b + 1) * rows, :].astype(f32), b * rows, 1)
    numbers = numbers[layer * top : (layer + 1) * top, :]
    shares = numbers / jnp.maximum(jnp.sum(numbers, axis=0, keepdims=True), 1.0)
    for j in range(exp_host):
        weight = jnp.sum(mask_ref[layer, j] * shares, axis=0, keepdims=True)
        gate = acc_ref[0, j * units : (j + 1) * units, :] * scale
        up = acc_ref[1, j * units : (j + 1) * units, :] * scale
        hidden = gate / (1.0 + jnp.exp(-gate)) * up * weight
        out_ref[j * tokens : (j + 1) * tokens, :] = hidden.T[:tokens].astype(bf16)


def down_kernel(*refs, layer, shards, exp_host, units, width, tokens):
    h_refs = refs[:shards]
    down_hbm, own_ref, send_ref, down_buf, acc_ref, sems = refs[shards:]
    column = lax.axis_index("ep")
    pairs = shards // 2
    pair_units = 2 * units

    def copy(m):
        offset = pl.multiple_of(((column // 2) ^ m) * pair_units, lanes)
        return pltpu.make_async_copy(down_hbm.at[layer, :, :, pl.ds(offset, pair_units)], down_buf.at[m], sems.at[m])

    for m in range(pairs):
        copy(m).start()
    odd = column % 2 == 1
    for m in range(pairs):
        parts = []
        for j in range(exp_host):
            mine = h_refs[2 * m][j * tokens : (j + 1) * tokens, :].astype(f32)
            other = h_refs[2 * m + 1][j * tokens : (j + 1) * tokens, :].astype(f32)
            parts += [jnp.where(odd, other, mine), jnp.where(odd, mine, other)]
        hidden = jnp.concatenate(parts, axis=1).astype(bf16)
        copy(m).wait()
        weights = jnp.concatenate([down_buf[m, j] for j in range(exp_host)], axis=1)
        part = lax.dot_general(weights, hidden, (((1,), (1,)), ((), ())), preferred_element_type=f32)
        if m == 0:
            acc_ref[:, :tokens] = part
        else:
            acc_ref[:, :tokens] = acc_ref[:, :tokens] + part
    result = acc_ref[...].T[:tokens]
    own_ref[...] = result
    send_ref[...] = result.astype(bf16)


def vmem_spec():
    return pl.BlockSpec(memory_space=pltpu.VMEM)


def smem_spec():
    return pl.BlockSpec(memory_space=pltpu.SMEM)


def hbm_spec():
    return pl.BlockSpec(memory_space=pltpu.HBM)


def in_hbm(value):
    return pltpu.with_memory_space_constraint(value, pltpu.HBM)


def xor_permute(value, axis, size, bits):
    return lax.ppermute(value, axis, [(i, i ^ bits) for i in range(size)])


def gather_shards(value, size):
    same = {0: value}
    for k in sorted(range(2, size, 2), reverse=True):
        same[k] = xor_permute(value, "ep", size, k)
    both = {}
    for k, part in same.items():
        both[k] = part
        both[k + 1] = xor_permute(part, "ep", size, 1)
    return [both[k] for k in range(size)]


def fast_device(tokens, norm_gain, gate_weight, up_weight, down_weight, replica_plan, route_expert, replica_pick, combine_num):
    groups = lax.axis_size("dp")
    shards = lax.axis_size("ep")
    layers = norm_gain.shape[0]
    exp_host, units = gate_weight.shape[1:3]
    rep_host = replica_plan.shape[2]
    rows, width = tokens.shape
    count = groups * rows
    top = route_expert.shape[2]
    capacity = rows // 2
    sizes = (layers, groups, rows, top, exp_host, rep_host, capacity)

    numbers = combine_num.transpose(0, 2, 1).reshape(layers * top, rows).astype(bf16)
    numbers = jnp.pad(numbers, ((0, rows - layers * top), (0, lanes - rows)))
    payload = jnp.concatenate([tokens, numbers], axis=1)
    gathered = [payload] + [xor_permute(payload, "dp", groups, k) for k in range(1, groups)]
    gathered = jnp.concatenate(gathered, axis=0)
    stream = gathered[:, :width]
    number = gathered[:, width:]

    mask = pl.pallas_call(
        functools.partial(routing_kernel, sizes=sizes),
        out_shape=jax.ShapeDtypeStruct((layers, exp_host, top, lanes), f32),
        in_specs=[smem_spec(), vmem_spec(), vmem_spec()],
        out_specs=vmem_spec(),
        compiler_params=pltpu.CompilerParams(vmem_limit_bytes=8 * 2**20),
        name="routing",
    )(replica_plan.transpose(0, 2, 1), route_expert.transpose(0, 2, 1), replica_pick.transpose(0, 2, 1))

    for layer in range(layers):
        xs = gather_shards(stream, shards)
        hidden = pl.pallas_call(
            functools.partial(
                gate_kernel, layer=layer, top=top, rows=rows, shards=shards, exp_host=exp_host, units=units, width=width
            ),
            out_shape=jax.ShapeDtypeStruct((exp_host * count, units), bf16),
            in_specs=[vmem_spec()] * (3 + shards) + [hbm_spec()] * 2,
            out_specs=vmem_spec(),
            scratch_shapes=[
                pltpu.VMEM((shards // 2, exp_host, units, 2 * width), bf16),
                pltpu.VMEM((shards // 2, exp_host, units, 2 * width), bf16),
                pltpu.VMEM((2, exp_host * units, lanes), f32),
                pltpu.SemaphoreType.DMA((2, shards // 2)),
            ],
            compiler_params=pltpu.CompilerParams(vmem_limit_bytes=30 * 2**20),
            name=f"gate_up_{layer}",
        )(mask, number, norm_gain, *xs, in_hbm(gate_weight), in_hbm(up_weight))
        hs = gather_shards(hidden, shards)
        own, send = pl.pallas_call(
            functools.partial(
                down_kernel, layer=layer, shards=shards, exp_host=exp_host, units=units, width=width, tokens=count
            ),
            out_shape=(jax.ShapeDtypeStruct((count, width), f32), jax.ShapeDtypeStruct((count, width), bf16)),
            in_specs=[vmem_spec()] * shards + [hbm_spec()],
            out_specs=(vmem_spec(), vmem_spec()),
            scratch_shapes=[
                pltpu.VMEM((shards // 2, exp_host, width, 2 * units), bf16),
                pltpu.VMEM((width, lanes), f32),
                pltpu.SemaphoreType.DMA((shards // 2,)),
            ],
            compiler_params=pltpu.CompilerParams(vmem_limit_bytes=18 * 2**20),
            name=f"down_{layer}",
        )(*hs, in_hbm(down_weight))
        if layer + 1 < layers:
            update = own
            for k in range(1, groups):
                other = xor_permute(send, "dp", groups, k).astype(f32)
                blocks = [other[(b ^ k) * rows : ((b ^ k) + 1) * rows] for b in range(groups)]
                update = update + jnp.concatenate(blocks, axis=0)
        else:
            update = own[:rows]
            for k in range(1, groups):
                update = update + xor_permute(send[k * rows : (k + 1) * rows], "dp", groups, k).astype(f32)
            stream = stream[:rows]
        stream = (stream.astype(f32) + update).astype(bf16)
    return stream, update.astype(bf16)


def serve_table(plan_layer, groups, exp_host, rep_host):
    replicas = exp_host + rep_host
    flat = jnp.arange(groups * replicas, dtype=jnp.int32)
    host_of = flat // replicas
    local = flat % replicas
    copy = jnp.clip(local - exp_host, 0, rep_host - 1)
    copied = ((host_of - 1 - copy) % groups) * exp_host + plan_layer[host_of, copy]
    return jnp.where(local < exp_host, host_of * exp_host + local, copied)


def kept_slots(experts, picks, table, capacity):
    flat_e = experts.reshape(-1)
    matches = (table[None, :] == flat_e[:, None]).astype(jnp.int32)
    rank = jnp.cumsum(matches, axis=1) - 1
    wanted = picks.reshape(-1) % jnp.sum(matches, axis=1)
    chosen = matches * (rank == wanted[:, None]).astype(jnp.int32)
    before = jnp.cumsum(chosen, axis=0) - chosen
    return (jnp.sum(before * chosen, axis=1) < capacity).reshape(experts.shape)


def plain_device(tokens, norm_gain, gate_weight, up_weight, down_weight, replica_plan, route_expert, replica_pick, combine_num):
    groups = lax.axis_size("dp")
    host = lax.axis_index("dp")
    layers, full = norm_gain.shape
    exp_host = gate_weight.shape[1]
    rep_host = replica_plan.shape[2]
    rows, width = tokens.shape
    count = groups * rows
    top = route_expert.shape[2]
    stream = lax.all_gather(tokens, "dp", axis=0, tiled=True)
    numbers = lax.all_gather(combine_num, "dp", axis=1, tiled=True).astype(f32)
    own_ids = host * exp_host + jnp.arange(exp_host, dtype=jnp.int32)
    for layer in range(layers):
        table = serve_table(replica_plan[layer], groups, exp_host, rep_host)
        kept = jax.vmap(lambda e, p: kept_slots(e, p, table, rows // 2))(
            route_expert[layer].reshape(groups, rows, top), replica_pick[layer].reshape(groups, rows, top)
        ).reshape(count, top)
        weights = numbers[layer] / jnp.sum(numbers[layer], axis=1, keepdims=True) * kept
        hits = route_expert[layer][:, :, None] == own_ids[None, None, :]
        combine = jnp.sum(weights[:, :, None] * hits, axis=1)
        whole = lax.all_gather(stream, "ep", axis=1, tiled=True).astype(f32)
        inverse = lax.rsqrt(jnp.mean(whole * whole, axis=1, keepdims=True) + epsilon)
        normed = (whole * inverse * norm_gain[layer][None, :]).astype(bf16)
        gate = jnp.einsum("nd,rfd->rnf", normed, gate_weight[layer], preferred_element_type=f32)
        up = jnp.einsum("nd,rfd->rnf", normed, up_weight[layer], preferred_element_type=f32)
        hidden = (jax.nn.silu(gate) * up * combine.T[:, :, None]).astype(bf16)
        hidden = lax.all_gather(hidden, "ep", axis=2, tiled=True)
        partial = jnp.einsum("rnf,rdf->nd", hidden, down_weight[layer], preferred_element_type=f32)
        parts = lax.all_gather(partial.astype(bf16), "dp", axis=0).astype(f32)
        update = jnp.sum(parts, axis=0)
        stream = (stream.astype(f32) + update).astype(bf16)
    stream = lax.dynamic_slice_in_dim(stream, host * rows, rows, 0)
    update = lax.dynamic_slice_in_dim(update, host * rows, rows, 0)
    return stream, update.astype(bf16)


def per_device(*args):
    tokens, norm_gain, gate_weight = args[:3]
    groups, shards = lax.axis_size("dp"), lax.axis_size("ep")
    layers, units = norm_gain.shape[0], gate_weight.shape[2]
    rows, width = tokens.shape
    fits = (
        groups & (groups - 1) == 0
        and shards & (shards - 1) == 0
        and 2 <= shards <= 8
        and width % lanes == 0
        and units % lanes == 0
        and rows % 16 == 0
        and groups * rows <= lanes
        and layers * args[6].shape[2] <= rows
        and args[6].shape[2] % 8 == 0
    )
    return fast_device(*args) if fits else plain_device(*args)


def solution(mesh):
    return jax.shard_map(
        per_device,
        mesh=mesh,
        in_specs=(
            P("dp", "ep"),
            P(),
            P(None, "dp", "ep", None),
            P(None, "dp", "ep", None),
            P(None, "dp", "ep", None),
            P(),
            P(),
            P(),
            P(None, "dp", None),
        ),
        out_specs=(P("dp", "ep"), P("dp", "ep")),
        check_vma=False,
    )
```

```python
import functools

import jax
import jax.numpy as jnp
from jax import lax
from jax.experimental import pallas as pl
from jax.experimental.pallas import tpu as pltpu
from jax.sharding import PartitionSpec as P


epsilon = 1e-06
lanes = 128
widest = 8
bf16 = jnp.bfloat16
f32 = jnp.float32


def routing(plan_ref, route_ref, pick_ref, mask_ref, sizes):
    layers, groups, rows, top, exp_host, rep_host, capacity = sizes
    host = lax.axis_index("dp")
    replicas = exp_host + rep_host
    tokens = groups * rows
    slots = -(-groups * replicas // 8) * 8
    slot_i = lax.broadcasted_iota(jnp.int32, (slots, 1), 0)
    from_i = lax.broadcasted_iota(jnp.int32, (tokens, lanes), 0)
    to_i = lax.broadcasted_iota(jnp.int32, (tokens, lanes), 1)
    earlier = jnp.where((from_i // rows == to_i // rows) & (from_i < to_i), 1.0, 0.0).astype(bf16)[:, :tokens]
    swap = jnp.where((from_i // rows == (to_i // rows) ^ host) & (from_i % rows == to_i % rows), 1.0, 0.0).astype(bf16)
    for layer in range(layers):
        served = []
        for slot in range(groups * replicas):
            owner, local = divmod(slot, replicas)
            if local < exp_host:
                served.append(owner * exp_host + local)
            else:
                copy = local - exp_host
                served.append(((owner - 1 - copy) % groups) * exp_host + plan_ref[layer, copy, owner])
        table = jnp.full((slots, 1), -1, jnp.int32)
        for slot, expert in enumerate(served):
            table = jnp.where(slot_i == slot, expert, table)
        rank = jnp.zeros((slots, 1), f32)
        count = jnp.zeros((slots, 1), f32)
        for slot, expert in enumerate(served):
            same = jnp.where(table == expert, 1.0, 0.0)
            count = count + same
            rank = rank + jnp.where(slot_i > slot, same, 0.0)
        count = jnp.broadcast_to(jnp.maximum(count, 1.0), (slots, tokens))
        rank = jnp.broadcast_to(rank, (slots, tokens))
        table = jnp.broadcast_to(table, (slots, tokens))
        experts = route_ref[layer]
        picks = pick_ref[layer].astype(f32)
        chosen = []
        for k in range(top):
            pick = picks[k : k + 1, :]
            wanted = pick - count * jnp.floor((pick + 0.5) / count)
            chosen.append(jnp.where((experts[k : k + 1, :] == table) & (rank == wanted), 1.0, 0.0))
        total = functools.reduce(lambda a, b: a + b, chosen)
        before = jnp.dot(total.astype(bf16), earlier, preferred_element_type=f32)
        kept = []
        for k in range(top):
            position = jnp.sum(before * chosen[k], axis=0, keepdims=True)
            before = before + chosen[k]
            kept.append(jnp.where(position < capacity - 0.5, 1.0, 0.0))
        kept = jnp.concatenate(kept, axis=0)
        for j in range(exp_host):
            mask = jnp.where(experts == host * exp_host + j, kept, 0.0)
            mask_ref[layer, j] = jnp.dot(mask.astype(bf16), swap, preferred_element_type=f32)


def setup_kernel(
    _, plan_hbm, route_hbm, pick_hbm, gain_hbm, weight_hbm, mask_ref, gain_ref, weight_ref, plan_ref, route_ref, pick_ref, sems, *, sizes
):
    small = [(plan_hbm, plan_ref), (route_hbm, route_ref), (pick_hbm, pick_ref), (gain_hbm, gain_ref)]
    moves = [pltpu.make_async_copy(src, dst, sems.at[i]) for i, (src, dst) in enumerate(small)]
    moves.append(pltpu.make_async_copy(weight_hbm.at[0], weight_ref, sems.at[len(small)]))
    for move in moves:
        move.start()
    for move in moves[:3]:
        move.wait()
    routing(plan_ref, route_ref, pick_ref, mask_ref, sizes)
    for move in moves[3:]:
        move.wait()


def prefetch_kernel(*refs, layer, count):
    sources, results, sems = refs[-2 * count - 1 : -count - 1], refs[-count - 1 : -1], refs[-1]
    moves = [
        pltpu.make_async_copy(src.at[layer], dst, sems.at[i]) for i, (src, dst) in enumerate(zip(sources, results))
    ]
    for move in moves:
        move.start()
    for move in moves:
        move.wait()


def gate_kernel(mask_ref, num_ref, gain_ref, *refs, layer, top, rows, shards, exp_host, units, width):
    x_refs = refs[:shards]
    gate_ref, up_ref, out_ref, acc_ref = refs[shards:]
    column = lax.axis_index("ep")
    pairs = shards // 2
    pair_width = 2 * width
    full = shards * width
    tokens = x_refs[0].shape[0]
    odd = column % 2 == 1
    squares = jnp.zeros((tokens, 1), f32)
    for m in range(pairs):
        mine = x_refs[2 * m][...].astype(f32)
        other = x_refs[2 * m + 1][...].astype(f32)
        squares = squares + jnp.sum(mine * mine + other * other, axis=1, keepdims=True)
        both = jnp.concatenate([jnp.where(odd, other, mine), jnp.where(odd, mine, other)], axis=1)
        offset = pl.multiple_of(((column // 2) ^ m) * pair_width, lanes)
        gain = gain_ref[layer : layer + 1, pl.ds(offset, pair_width)]
        scaled = (both * gain).astype(bf16)
        for i, weight_ref in enumerate((gate_ref, up_ref)):
            part = lax.dot_general(
                weight_ref[:, :, pl.ds(offset, pair_width)].reshape(exp_host * units, pair_width),
                scaled,
                (((1,), (1,)), ((), ())),
                preferred_element_type=f32,
            )
            if m == 0:
                acc_ref[i, :, :tokens] = part
            else:
                acc_ref[i, :, :tokens] = acc_ref[i, :, :tokens] + part
    inverse = lax.rsqrt(squares / full + epsilon)
    turned = jnp.concatenate([jnp.broadcast_to(inverse, (tokens, lanes)), jnp.zeros((lanes - tokens, lanes), f32)], axis=0).T
    scale = turned[0:1, :]
    blocks = num_ref.shape[0] // rows
    numbers = num_ref[0:rows, :].astype(f32)
    for b in range(1, blocks):
        numbers = numbers + pltpu.roll(num_ref[b * rows : (b + 1) * rows, :].astype(f32), b * rows, 1)
    numbers = numbers[layer * top : (layer + 1) * top, :]
    shares = numbers / jnp.maximum(jnp.sum(numbers, axis=0, keepdims=True), 1.0)
    for j in range(exp_host):
        weight = jnp.sum(mask_ref[layer, j] * shares, axis=0, keepdims=True)
        gate = acc_ref[0, j * units : (j + 1) * units, :] * scale
        up = acc_ref[1, j * units : (j + 1) * units, :] * scale
        hidden = gate / (1.0 + jnp.exp(-gate)) * up * weight
        out_ref[j * tokens : (j + 1) * tokens, :] = hidden.T[:tokens].astype(bf16)


def down_kernel(*refs, layer, shards, exp_host, units, width, tokens):
    h_refs = refs[:shards]
    down_ref, own_ref, send_ref, acc_ref = refs[shards:]
    column = lax.axis_index("ep")
    pairs = shards // 2
    pair_units = 2 * units
    odd = column % 2 == 1
    for m in range(pairs):
        parts = []
        for j in range(exp_host):
            mine = h_refs[2 * m][j * tokens : (j + 1) * tokens, :].astype(f32)
            other = h_refs[2 * m + 1][j * tokens : (j + 1) * tokens, :].astype(f32)
            parts += [jnp.where(odd, other, mine), jnp.where(odd, mine, other)]
        hidden = jnp.concatenate(parts, axis=1).astype(bf16)
        offset = pl.multiple_of(((column // 2) ^ m) * pair_units, lanes)
        weights = jnp.concatenate([down_ref[j, :, pl.ds(offset, pair_units)] for j in range(exp_host)], axis=1)
        part = lax.dot_general(weights, hidden, (((1,), (1,)), ((), ())), preferred_element_type=f32)
        if m == 0:
            acc_ref[:, :tokens] = part
        else:
            acc_ref[:, :tokens] = acc_ref[:, :tokens] + part
    result = acc_ref[...].T[:tokens]
    own_ref[...] = result
    send_ref[...] = result.astype(bf16)


def vmem_spec():
    return pl.BlockSpec(memory_space=pltpu.VMEM)


def hbm_spec():
    return pl.BlockSpec(memory_space=pltpu.HBM)


def any_spec():
    return pl.BlockSpec(memory_space=pl.ANY)


def in_hbm(value):
    return pltpu.with_memory_space_constraint(value, pltpu.HBM)


def prefetch(layer, after, *weights):
    size = sum(w.size // w.shape[0] * w.dtype.itemsize for w in weights)
    return pl.pallas_call(
        functools.partial(prefetch_kernel, layer=layer, count=len(weights)),
        out_shape=tuple(pltpu.VMEM(w.shape[1:], w.dtype) for w in weights),
        in_specs=[any_spec()] + [hbm_spec()] * len(weights),
        out_specs=tuple(vmem_spec() for _ in weights),
        scratch_shapes=[pltpu.SemaphoreType.DMA((len(weights),))],
        compiler_params=pltpu.CompilerParams(vmem_limit_bytes=2**20),
        cost_estimate=pl.CostEstimate(flops=400 * size, bytes_accessed=2 * size, transcendentals=0),
    )(after, *[in_hbm(w) for w in weights])


def xor_permute(value, axis, size, bits):
    return lax.ppermute(value, axis, [(i, i ^ bits) for i in range(size)])


def gather_shards(value, size):
    same = {0: value}
    for k in sorted(range(2, size, 2), reverse=True):
        same[k] = xor_permute(value, "ep", size, k)
    both = {}
    for k, part in same.items():
        both[k] = part
        both[k + 1] = xor_permute(part, "ep", size, 1)
    return [both[k] for k in range(size)]


def fast_device(tokens, norm_gain, gate_weight, up_weight, down_weight, replica_plan, route_expert, replica_pick, combine_num):
    groups = lax.axis_size("dp")
    shards = lax.axis_size("ep")
    layers = norm_gain.shape[0]
    exp_host, units = gate_weight.shape[1:3]
    rep_host = replica_plan.shape[2]
    rows, width = tokens.shape
    count = groups * rows
    top = route_expert.shape[2]
    capacity = rows // 2
    sizes = (layers, groups, rows, top, exp_host, rep_host, capacity)

    numbers = combine_num.transpose(0, 2, 1).reshape(layers * top, rows).astype(bf16)
    numbers = jnp.pad(numbers, ((0, rows - layers * top), (0, lanes - rows)))
    payload = jnp.concatenate([tokens, numbers], axis=1)
    gathered = [payload]
    (ups,) = prefetch(0, payload, up_weight)
    for k in range(1, groups):
        gathered.append(xor_permute(payload, "dp", groups, k))
    gathered = jnp.concatenate(gathered, axis=0)
    stream = gathered[:, :width]
    number = gathered[:, width:]

    prepare = pl.pallas_call(
        functools.partial(setup_kernel, sizes=sizes),
        out_shape=(
            pltpu.VMEM((layers, exp_host, top, lanes), f32),
            pltpu.VMEM(norm_gain.shape, f32),
            pltpu.VMEM(gate_weight.shape[1:], bf16),
        ),
        in_specs=[any_spec()] + [hbm_spec()] * 5,
        out_specs=(vmem_spec(),) * 3,
        scratch_shapes=[
            pltpu.SMEM((layers, rep_host, groups), jnp.int32),
            pltpu.VMEM((layers, top, count), jnp.int32),
            pltpu.VMEM((layers, top, count), jnp.int32),
            pltpu.SemaphoreType.DMA((5,)),
        ],
        compiler_params=pltpu.CompilerParams(vmem_limit_bytes=4 * 2**20),
        cost_estimate=pl.CostEstimate(flops=4 * 10**9, bytes_accessed=2 * 10**7, transcendentals=0),
        name="setup",
    )
    small = (replica_plan, route_expert, replica_pick)
    small = [in_hbm(v.transpose(0, 2, 1)) for v in small] + [in_hbm(norm_gain), in_hbm(gate_weight)]
    mask, gains, gates = prepare(stream, *small)

    for layer in range(layers):
        xs = gather_shards(stream, shards)
        hidden = pl.pallas_call(
            functools.partial(
                gate_kernel, layer=layer, top=top, rows=rows, shards=shards, exp_host=exp_host, units=units, width=width
            ),
            out_shape=jax.ShapeDtypeStruct((exp_host * count, units), bf16),
            in_specs=[vmem_spec()] * (5 + shards),
            out_specs=vmem_spec(),
            scratch_shapes=[
                pltpu.VMEM((2, exp_host * units, lanes), f32),
            ],
            compiler_params=pltpu.CompilerParams(vmem_limit_bytes=8 * 2**20),
        )(mask, number, gains, *xs, gates, ups)
        (downs,) = prefetch(layer, hidden, down_weight)
        hs = gather_shards(hidden, shards)
        own, send = pl.pallas_call(
            functools.partial(
                down_kernel, layer=layer, shards=shards, exp_host=exp_host, units=units, width=width, tokens=count
            ),
            out_shape=(jax.ShapeDtypeStruct((count, width), f32), jax.ShapeDtypeStruct((count, width), bf16)),
            in_specs=[vmem_spec()] * (shards + 1),
            out_specs=(vmem_spec(), vmem_spec()),
            scratch_shapes=[
                pltpu.VMEM((width, lanes), f32),
            ],
            compiler_params=pltpu.CompilerParams(vmem_limit_bytes=8 * 2**20),
        )(*hs, downs)
        if layer + 1 < layers:
            gates, ups = prefetch(layer + 1, send, gate_weight, up_weight)
            update = own
            for k in range(1, groups):
                other = xor_permute(send, "dp", groups, k).astype(f32)
                blocks = [other[(b ^ k) * rows : ((b ^ k) + 1) * rows] for b in range(groups)]
                update = update + jnp.concatenate(blocks, axis=0)
        else:
            update = own[:rows]
            for k in range(1, groups):
                update = update + xor_permute(send[k * rows : (k + 1) * rows], "dp", groups, k).astype(f32)
            stream = stream[:rows]
        stream = (stream.astype(f32) + update).astype(bf16)
    return stream, update.astype(bf16)


def serve_table(plan_layer, groups, exp_host, rep_host):
    replicas = exp_host + rep_host
    flat = jnp.arange(groups * replicas, dtype=jnp.int32)
    host_of = flat // replicas
    local = flat % replicas
    copy = jnp.clip(local - exp_host, 0, rep_host - 1)
    copied = ((host_of - 1 - copy) % groups) * exp_host + plan_layer[host_of, copy]
    return jnp.where(local < exp_host, host_of * exp_host + local, copied)


def kept_slots(experts, picks, table, capacity):
    flat_e = experts.reshape(-1)
    matches = (table[None, :] == flat_e[:, None]).astype(jnp.int32)
    rank = jnp.cumsum(matches, axis=1) - 1
    wanted = picks.reshape(-1) % jnp.sum(matches, axis=1)
    chosen = matches * (rank == wanted[:, None]).astype(jnp.int32)
    before = jnp.cumsum(chosen, axis=0) - chosen
    return (jnp.sum(before * chosen, axis=1) < capacity).reshape(experts.shape)


def plain_device(tokens, norm_gain, gate_weight, up_weight, down_weight, replica_plan, route_expert, replica_pick, combine_num):
    groups = lax.axis_size("dp")
    host = lax.axis_index("dp")
    layers, _ = norm_gain.shape
    exp_host = gate_weight.shape[1]
    rep_host = replica_plan.shape[2]
    rows, _ = tokens.shape
    count = groups * rows
    top = route_expert.shape[2]
    stream = lax.all_gather(tokens, "dp", axis=0, tiled=True)
    numbers = lax.all_gather(combine_num, "dp", axis=1, tiled=True).astype(f32)
    own_ids = host * exp_host + jnp.arange(exp_host, dtype=jnp.int32)
    for layer in range(layers):
        table = serve_table(replica_plan[layer], groups, exp_host, rep_host)
        kept = jax.vmap(lambda e, p: kept_slots(e, p, table, rows // 2))(
            route_expert[layer].reshape(groups, rows, top), replica_pick[layer].reshape(groups, rows, top)
        ).reshape(count, top)
        weights = numbers[layer] / jnp.sum(numbers[layer], axis=1, keepdims=True) * kept
        hits = route_expert[layer][:, :, None] == own_ids[None, None, :]
        combine = jnp.sum(weights[:, :, None] * hits, axis=1)
        whole = lax.all_gather(stream, "ep", axis=1, tiled=True).astype(f32)
        inverse = lax.rsqrt(jnp.mean(whole * whole, axis=1, keepdims=True) + epsilon)
        normed = (whole * inverse * norm_gain[layer][None, :]).astype(bf16)
        gate = jnp.einsum("nd,rfd->rnf", normed, gate_weight[layer], preferred_element_type=f32)
        up = jnp.einsum("nd,rfd->rnf", normed, up_weight[layer], preferred_element_type=f32)
        hidden = (jax.nn.silu(gate) * up * combine.T[:, :, None]).astype(bf16)
        hidden = lax.all_gather(hidden, "ep", axis=2, tiled=True)
        partial = jnp.einsum("rnf,rdf->nd", hidden, down_weight[layer], preferred_element_type=f32)
        parts = lax.all_gather(partial.astype(bf16), "dp", axis=0).astype(f32)
        update = jnp.sum(parts, axis=0)
        stream = (stream.astype(f32) + update).astype(bf16)
    stream = lax.dynamic_slice_in_dim(stream, host * rows, rows, 0)
    update = lax.dynamic_slice_in_dim(update, host * rows, rows, 0)
    return stream, update.astype(bf16)


def per_device(*args):
    tokens, norm_gain, gate_weight = args[:3]
    groups, shards = lax.axis_size("dp"), lax.axis_size("ep")
    layers, units = norm_gain.shape[0], gate_weight.shape[2]
    rows, width = tokens.shape
    fits = (
        groups & (groups - 1) == 0
        and shards & (shards - 1) == 0
        and 2 <= shards <= widest
        and width % lanes == 0
        and units % lanes == 0
        and rows % 16 == 0
        and groups * rows <= lanes
        and layers * args[6].shape[2] <= rows
        and args[6].shape[2] % 8 == 0
    )
    return fast_device(*args) if fits else plain_device(*args)


def solution(mesh):
    return jax.shard_map(
        per_device,
        mesh=mesh,
        in_specs=(
            P("dp", "ep"),
            P(),
            P(None, "dp", "ep", None),
            P(None, "dp", "ep", None),
            P(None, "dp", "ep", None),
            P(),
            P(),
            P(),
            P(None, "dp", None),
        ),
        out_specs=(P("dp", "ep"), P("dp", "ep")),
        check_vma=False,
    )
```

```python
import functools

import jax
import jax.numpy as jnp
from jax import lax
from jax.experimental import pallas as pl
from jax.experimental.pallas import tpu as pltpu
from jax.sharding import PartitionSpec as P


epsilon = 1e-06
lanes = 128
widest = 8
bf16 = jnp.bfloat16
f32 = jnp.float32


def routing(plan_ref, route_ref, pick_ref, mask_ref, sizes):
    layers, groups, rows, top, exp_host, rep_host, capacity = sizes
    host = lax.axis_index("dp")
    replicas = exp_host + rep_host
    tokens = groups * rows
    slots = -(-groups * replicas // 8) * 8
    slot_i = lax.broadcasted_iota(jnp.int32, (slots, 1), 0)
    from_i = lax.broadcasted_iota(jnp.int32, (tokens, lanes), 0)
    to_i = lax.broadcasted_iota(jnp.int32, (tokens, lanes), 1)
    earlier = jnp.where((from_i // rows == to_i // rows) & (from_i < to_i), 1.0, 0.0).astype(bf16)[:, :tokens]
    swap = jnp.where((from_i // rows == (to_i // rows) ^ host) & (from_i % rows == to_i % rows), 1.0, 0.0).astype(bf16)
    for layer in range(layers):
        served = []
        for slot in range(groups * replicas):
            owner, local = divmod(slot, replicas)
            if local < exp_host:
                served.append(owner * exp_host + local)
            else:
                copy = local - exp_host
                served.append(((owner - 1 - copy) % groups) * exp_host + plan_ref[layer, copy, owner])
        table = jnp.full((slots, 1), -1, jnp.int32)
        for slot, expert in enumerate(served):
            table = jnp.where(slot_i == slot, expert, table)
        rank = jnp.zeros((slots, 1), f32)
        count = jnp.zeros((slots, 1), f32)
        for slot, expert in enumerate(served):
            same = jnp.where(table == expert, 1.0, 0.0)
            count = count + same
            rank = rank + jnp.where(slot_i > slot, same, 0.0)
        count = jnp.broadcast_to(jnp.maximum(count, 1.0), (slots, tokens))
        rank = jnp.broadcast_to(rank, (slots, tokens))
        table = jnp.broadcast_to(table, (slots, tokens))
        experts = route_ref[layer]
        picks = pick_ref[layer].astype(f32)
        chosen = []
        for k in range(top):
            pick = picks[k : k + 1, :]
            wanted = pick - count * jnp.floor((pick + 0.5) / count)
            chosen.append(jnp.where((experts[k : k + 1, :] == table) & (rank == wanted), 1.0, 0.0))
        total = functools.reduce(lambda a, b: a + b, chosen)
        before = jnp.dot(total.astype(bf16), earlier, preferred_element_type=f32)
        kept = []
        for k in range(top):
            position = jnp.sum(before * chosen[k], axis=0, keepdims=True)
            before = before + chosen[k]
            kept.append(jnp.where(position < capacity - 0.5, 1.0, 0.0))
        kept = jnp.concatenate(kept, axis=0)
        for j in range(exp_host):
            mask = jnp.where(experts == host * exp_host + j, kept, 0.0)
            mask_ref[layer, j] = jnp.dot(mask.astype(bf16), swap, preferred_element_type=f32)


def slabs(source, target, ks, size, sems):
    column = lax.axis_index("ep")
    moves = []
    for i, k in enumerate(ks):
        block = pl.ds(pl.multiple_of((column ^ k) * size, lanes), size)
        moves.append(pltpu.make_async_copy(source.at[:, :, block], target.at[:, :, block], sems.at[i]))
    return moves


def setup_kernel(
    x_ref, ups_ref, plan_hbm, route_hbm, pick_hbm, gain_hbm, weight_hbm, mask_ref, gain_ref, weight_ref, sums_ref, total_ref,
    plan_ref, route_ref, pick_ref, sems, slab_sems, *, sizes, shards, units, width,
):
    small = [(plan_hbm, plan_ref), (route_hbm, route_ref), (pick_hbm, pick_ref)]
    small.append((gain_hbm, gain_ref.at[:, pl.ds(0, gain_hbm.shape[1])]))
    moves = [pltpu.make_async_copy(src, dst, sems.at[i]) for i, (src, dst) in enumerate(small)]
    heavy = slabs(weight_hbm.at[0], weight_ref, range(shards), width, slab_sems)
    for move in moves + heavy:
        move.start()
    for move in moves[:3]:
        move.wait()
    routing(plan_ref, route_ref, pick_ref, mask_ref, sizes)
    moves[3].wait()
    heavy[0].wait()
    squares, sums = feature_sums((weight_ref, ups_ref), gain_ref, [x_ref], (0,), 0, sizes[4], units, width)
    tokens = x_ref.shape[0]
    for i, part in enumerate(sums):
        sums_ref[i, :, :tokens] = part
    total_ref[...] = jnp.broadcast_to(squares, (tokens, lanes))
    for move in heavy[1:]:
        move.wait()


def early_kernel(_, weight_hbm, result_ref, sems, *, ks, width):
    moves = slabs(weight_hbm.at[0], result_ref, ks, width, sems)
    for move in moves:
        move.start()
    for move in moves:
        move.wait()


def early(after, weight, ks, width):
    return pl.pallas_call(
        functools.partial(early_kernel, ks=ks, width=width),
        out_shape=pltpu.VMEM(weight.shape[1:], weight.dtype),
        in_specs=[any_spec(), hbm_spec()],
        out_specs=vmem_spec(),
        scratch_shapes=[pltpu.SemaphoreType.DMA((len(ks),))],
        compiler_params=pltpu.CompilerParams(vmem_limit_bytes=2**20),
        cost_estimate=pl.CostEstimate(flops=4 * 10**9, bytes_accessed=2 * 10**7, transcendentals=0),
        name="early",
    )(after, in_hbm(weight))


def prefetch_kernel(*refs, layer, count):
    sources, results, sems = refs[-2 * count - 1 : -count - 1], refs[-count - 1 : -1], refs[-1]
    moves = [
        pltpu.make_async_copy(src.at[layer], dst, sems.at[i]) for i, (src, dst) in enumerate(zip(sources, results))
    ]
    for move in moves:
        move.start()
    for move in moves:
        move.wait()


def feature_sums(weight_refs, gain_ref, x_refs, ks, layer, exp_host, units, width):
    column = lax.axis_index("ep")
    offsets = [pl.multiple_of((column ^ k) * width, lanes) for k in ks]
    squares, scaled = 0.0, []
    for x_ref, offset in zip(x_refs, offsets):
        x = x_ref[...].astype(f32)
        squares = squares + jnp.sum(x * x, axis=1, keepdims=True)
        scaled.append((x * gain_ref[layer : layer + 1, pl.ds(offset, width)]).astype(bf16))
    scaled = jnp.concatenate(scaled, axis=1)
    sums = []
    for weight_ref in weight_refs:
        weight = jnp.concatenate([weight_ref[:, :, pl.ds(offset, width)] for offset in offsets], axis=2)
        weight = weight.reshape(exp_host * units, len(ks) * width)
        sums.append(lax.dot_general(weight, scaled, (((1,), (1,)), ((), ())), preferred_element_type=f32))
    return squares, sums


def gate_part(*refs, layer, ks, first, last, fill, top, rows, shards, exp_host, units, width):
    refs = list(refs)
    gate_ref, up_ref, gain_ref = refs[:3]
    x_refs = refs[3 : 3 + len(ks)]
    refs = refs[3 + len(ks) :]
    moves = []
    if not first:
        sums_ref, squares_ref = refs[:2]
        refs = refs[2:]
    if fill:
        source = refs.pop(0)
        sems = refs.pop()
        up_ref = refs.pop()
        moves = slabs(source.at[layer], up_ref, fill, width, sems)
        for move in moves:
            move.start()
    if last:
        mask_ref, num_ref, out_ref, acc_ref = refs
    else:
        acc_ref, total_ref = refs
    tokens = x_refs[0].shape[0]
    squares, sums = feature_sums((gate_ref, up_ref), gain_ref, x_refs, ks, layer, exp_host, units, width)
    if not first:
        squares = squares + squares_ref[:, 0:1]
    for i, part in enumerate(sums):
        acc_ref[i, :, :tokens] = part if first else sums_ref[i, :, :tokens] + part
    for move in moves:
        move.wait()
    if not last:
        total_ref[...] = jnp.broadcast_to(squares, (tokens, lanes))
        return
    inverse = lax.rsqrt(squares / (shards * width) + epsilon)
    turned = jnp.concatenate([jnp.broadcast_to(inverse, (tokens, lanes)), jnp.zeros((lanes - tokens, lanes), f32)], axis=0).T
    scale = turned[0:1, :]
    numbers = num_ref[0:rows, :].astype(f32)
    for b in range(1, num_ref.shape[0] // rows):
        numbers = numbers + pltpu.roll(num_ref[b * rows : (b + 1) * rows, :].astype(f32), b * rows, 1)
    numbers = numbers[layer * top : (layer + 1) * top, :]
    shares = numbers / jnp.maximum(jnp.sum(numbers, axis=0, keepdims=True), 1.0)
    for j in range(exp_host):
        weight = jnp.sum(mask_ref[layer, j] * shares, axis=0, keepdims=True)
        gate = acc_ref[0, j * units : (j + 1) * units, :] * scale
        up = acc_ref[1, j * units : (j + 1) * units, :] * scale
        hidden = gate / (1.0 + jnp.exp(-gate)) * up * weight
        out_ref[j * tokens : (j + 1) * tokens, :] = hidden.T[:tokens].astype(bf16)


def gate_up(layer, ks, gates, ups, gains, xs, sums, finish, sizes, units, width, shards, load=None, fill=()):
    _, groups, rows, top, exp_host, _, _ = sizes
    count = groups * rows
    sums_shape = pltpu.VMEM((2, exp_host * units, lanes), f32)
    last = finish is not None
    operands = [gates, ups, gains] + [xs[k] for k in ks] + list(sums or ()) + list(finish or ())
    in_specs = [vmem_spec()] * len(operands)
    out_shape = [pltpu.VMEM((exp_host * count, units), bf16)] if last else [sums_shape, pltpu.VMEM((count, lanes), f32)]
    scratch = [sums_shape] if last else []
    aliases = {}
    if load is not None:
        operands.append(in_hbm(load))
        in_specs.append(hbm_spec())
        out_shape.append(pltpu.VMEM(load.shape[1:], load.dtype))
        scratch.append(pltpu.SemaphoreType.DMA((len(fill),)))
        aliases = {1: len(out_shape) - 1}
    work = 2 * 2 * exp_host * units * width * len(ks) * count
    return pl.pallas_call(
        functools.partial(
            gate_part,
            layer=layer,
            ks=ks,
            first=sums is None,
            last=last,
            fill=fill,
            top=top,
            rows=rows,
            shards=shards,
            exp_host=exp_host,
            units=units,
            width=width,
        ),
        out_shape=out_shape,
        in_specs=in_specs,
        out_specs=[vmem_spec()] * len(out_shape),
        scratch_shapes=scratch,
        input_output_aliases=aliases,
        compiler_params=pltpu.CompilerParams(vmem_limit_bytes=8 * 2**20),
        cost_estimate=pl.CostEstimate(flops=work, bytes_accessed=work // count, transcendentals=0),
    )(*operands)


def down_part(*refs, ks, first, last, exp_host, units, tokens):
    down_ref = refs[0]
    h_refs = refs[1 : 1 + len(ks)]
    refs = refs[1 + len(ks) :]
    column = lax.axis_index("ep")
    parts, weights = [], []
    for h_ref, k in zip(h_refs, ks):
        offset = pl.multiple_of((column ^ k) * units, lanes)
        for j in range(exp_host):
            parts.append(h_ref[j * tokens : (j + 1) * tokens, :])
            weights.append(down_ref[j, :, pl.ds(offset, units)])
    part = lax.dot_general(
        jnp.concatenate(weights, axis=1),
        jnp.concatenate(parts, axis=1),
        (((1,), (1,)), ((), ())),
        preferred_element_type=f32,
    )
    if not first:
        part = refs[0][:, :tokens] + part
        refs = refs[1:]
    if not last:
        refs[0][:, :tokens] = part
        return
    own_ref, send_ref, acc_ref = refs
    acc_ref[:, :tokens] = part
    result = acc_ref[...].T[:tokens]
    own_ref[...] = result
    send_ref[...] = result.astype(bf16)


def down_first_kernel(h_ref, weight_hbm, weight_ref, sums_ref, sems, *, layer, shards, exp_host, units, tokens):
    moves = slabs(weight_hbm.at[layer], weight_ref, range(shards), units, sems)
    for move in moves:
        move.start()
    moves[0].wait()
    down_part(weight_ref, h_ref, sums_ref, ks=(0,), first=True, last=False, exp_host=exp_host, units=units, tokens=tokens)
    for move in moves[1:]:
        move.wait()


def down_first(layer, weight, hidden, shards, count, units, width, exp_host):
    return pl.pallas_call(
        functools.partial(
            down_first_kernel, layer=layer, shards=shards, exp_host=exp_host, units=units, tokens=count
        ),
        out_shape=[pltpu.VMEM(weight.shape[1:], weight.dtype), pltpu.VMEM((width, lanes), f32)],
        in_specs=[vmem_spec(), hbm_spec()],
        out_specs=[vmem_spec()] * 2,
        scratch_shapes=[pltpu.SemaphoreType.DMA((shards,))],
        compiler_params=pltpu.CompilerParams(vmem_limit_bytes=8 * 2**20),
        cost_estimate=pl.CostEstimate(flops=4 * 10**9, bytes_accessed=2 * 10**7, transcendentals=0),
    )(hidden, in_hbm(weight))


def down(ks, downs, hs, sums, last, count, units, width, exp_host):
    sums_shape = pltpu.VMEM((width, lanes), f32)
    operands = [downs] + [hs[k] for k in ks] + ([] if sums is None else [sums])
    work = 2 * exp_host * units * width * len(ks) * count
    return pl.pallas_call(
        functools.partial(
            down_part, ks=ks, first=sums is None, last=last, exp_host=exp_host, units=units, tokens=count
        ),
        out_shape=(pltpu.VMEM((count, width), f32), pltpu.VMEM((count, width), bf16)) if last else sums_shape,
        in_specs=[vmem_spec()] * len(operands),
        out_specs=(vmem_spec(), vmem_spec()) if last else vmem_spec(),
        scratch_shapes=[sums_shape] if last else [],
        compiler_params=pltpu.CompilerParams(vmem_limit_bytes=8 * 2**20),
        cost_estimate=pl.CostEstimate(flops=work, bytes_accessed=work // count, transcendentals=0),
    )(*operands)


def pack_kernel(tokens_hbm, numbers_hbm, out_ref, numbers_ref, sems, *, width):
    moves = [
        pltpu.make_async_copy(numbers_hbm, numbers_ref, sems.at[0]),
        pltpu.make_async_copy(tokens_hbm, out_ref.at[:, pl.ds(0, width)], sems.at[1]),
    ]
    for move in moves:
        move.start()
    layers, top, rows = numbers_ref.shape
    out_ref[:, width:] = jnp.zeros((out_ref.shape[0], lanes), bf16)
    moves[0].wait()
    numbers = jnp.concatenate([numbers_ref[layer] for layer in range(layers)], axis=0)
    out_ref[: layers * top, width : width + rows] = numbers.astype(f32).astype(bf16)
    moves[1].wait()


def pack(tokens, combine_num):
    rows, width = tokens.shape
    layers, _, top = combine_num.shape
    return pl.pallas_call(
        functools.partial(pack_kernel, width=width),
        out_shape=pltpu.VMEM((rows, width + lanes), bf16),
        in_specs=[hbm_spec()] * 2,
        out_specs=vmem_spec(),
        scratch_shapes=[pltpu.VMEM((layers, top, rows), jnp.int32), pltpu.SemaphoreType.DMA((2,))],
        compiler_params=pltpu.CompilerParams(vmem_limit_bytes=2**20),
        name="pack",
    )(in_hbm(tokens), in_hbm(combine_num.transpose(0, 2, 1)))


def vmem_spec():
    return pl.BlockSpec(memory_space=pltpu.VMEM)


def hbm_spec():
    return pl.BlockSpec(memory_space=pltpu.HBM)


def any_spec():
    return pl.BlockSpec(memory_space=pl.ANY)


def in_hbm(value):
    return pltpu.with_memory_space_constraint(value, pltpu.HBM)


def prefetch(layer, after, *weights):
    size = sum(w.size // w.shape[0] * w.dtype.itemsize for w in weights)
    return pl.pallas_call(
        functools.partial(prefetch_kernel, layer=layer, count=len(weights)),
        out_shape=tuple(pltpu.VMEM(w.shape[1:], w.dtype) for w in weights),
        in_specs=[any_spec()] + [hbm_spec()] * len(weights),
        out_specs=tuple(vmem_spec() for _ in weights),
        scratch_shapes=[pltpu.SemaphoreType.DMA((len(weights),))],
        compiler_params=pltpu.CompilerParams(vmem_limit_bytes=2**20),
        cost_estimate=pl.CostEstimate(flops=400 * size, bytes_accessed=2 * size, transcendentals=0),
    )(after, *[in_hbm(w) for w in weights])


def xor_permute(value, axis, size, bits):
    return lax.ppermute(value, axis, [(i, i ^ bits) for i in range(size)])


def gather_shards(value, size):
    same = {0: value}
    for k in sorted(range(2, size, 2), reverse=True):
        same[k] = xor_permute(value, "ep", size, k)
    both = {}
    for k, part in same.items():
        both[k] = part
        both[k + 1] = xor_permute(part, "ep", size, 1)
    return [both[k] for k in range(size)]


def fast_device(tokens, norm_gain, gate_weight, up_weight, down_weight, replica_plan, route_expert, replica_pick, combine_num):
    groups = lax.axis_size("dp")
    shards = lax.axis_size("ep")
    layers = norm_gain.shape[0]
    exp_host, units = gate_weight.shape[1:3]
    rep_host = replica_plan.shape[2]
    rows, width = tokens.shape
    count = groups * rows
    top = route_expert.shape[2]
    capacity = rows // 2
    sizes = (layers, groups, rows, top, exp_host, rep_host, capacity)

    same = tuple(range(0, shards, 2))
    late = tuple(k + 1 for k in same)
    payload = pack(tokens, combine_num)
    gathered = [payload]
    ups = early(payload, up_weight, same, width)
    for k in range(1, groups):
        gathered.append(xor_permute(payload, "dp", groups, k))
    gathered = jnp.concatenate(gathered, axis=0)
    stream = gathered[:, :width]
    number = gathered[:, width:]

    prepare = pl.pallas_call(
        functools.partial(setup_kernel, sizes=sizes, shards=shards, units=units, width=width),
        out_shape=(
            pltpu.VMEM((layers, exp_host, top, lanes), f32),
            pltpu.VMEM((layers, norm_gain.shape[1] + 4 * lanes), f32),
            pltpu.VMEM(gate_weight.shape[1:], bf16),
            pltpu.VMEM((2, exp_host * units, lanes), f32),
            pltpu.VMEM((count, lanes), f32),
        ),
        in_specs=[vmem_spec()] * 2 + [hbm_spec()] * 5,
        out_specs=(vmem_spec(),) * 5,
        scratch_shapes=[
            pltpu.SMEM((layers, rep_host, groups), jnp.int32),
            pltpu.VMEM((layers, top, count), jnp.int32),
            pltpu.VMEM((layers, top, count), jnp.int32),
            pltpu.SemaphoreType.DMA((4,)),
            pltpu.SemaphoreType.DMA((shards,)),
        ],
        compiler_params=pltpu.CompilerParams(vmem_limit_bytes=8 * 2**20),
        cost_estimate=pl.CostEstimate(flops=4 * 10**9, bytes_accessed=2 * 10**7, transcendentals=0),
        name="setup",
    )
    small = (replica_plan, route_expert, replica_pick)
    small = [in_hbm(v.transpose(0, 2, 1)) for v in small] + [in_hbm(norm_gain), in_hbm(gate_weight)]
    mask, gains, gates, *sums = prepare(stream, ups, *small)

    for layer in range(layers):
        xs = gather_shards(stream, shards)
        dims = (sizes, units, width, shards)
        finish = (mask, number)
        if layer == 0:
            *sums, ups = gate_up(layer, same[1:], gates, ups, gains, xs, sums, None, *dims, load=up_weight, fill=late)
            (hidden,) = gate_up(layer, late, gates, ups, gains, xs, sums, finish, *dims)
        else:
            sums = gate_up(layer, (0, 1), gates, ups, gains, xs, None, None, *dims)
            sums = gate_up(layer, same[1:], gates, ups, gains, xs, sums, None, *dims)
            (hidden,) = gate_up(layer, late[1:], gates, ups, gains, xs, sums, finish, *dims)
        hs = gather_shards(hidden, shards)
        dims = (count, units, width, exp_host)
        downs, sums = down_first(layer, down_weight, hidden, shards, *dims)
        sums = down(same[1:], downs, hs, sums, False, *dims)
        own, send = down(late, downs, hs, sums, True, *dims)
        if layer + 1 < layers:
            gates, ups = prefetch(layer + 1, send, gate_weight, up_weight)
            update = own
            for k in range(1, groups):
                other = xor_permute(send, "dp", groups, k).astype(f32)
                blocks = [other[(b ^ k) * rows : ((b ^ k) + 1) * rows] for b in range(groups)]
                update = update + jnp.concatenate(blocks, axis=0)
        else:
            update = own[:rows]
            for k in range(1, groups):
                other = xor_permute(send[k * rows : (k + 1) * rows], "dp", groups, k)
                update = update + other.astype(f32)
            stream = stream[:rows]
        stream = (stream.astype(f32) + update).astype(bf16)
    return stream, update.astype(bf16)


def serve_table(plan_layer, groups, exp_host, rep_host):
    replicas = exp_host + rep_host
    flat = jnp.arange(groups * replicas, dtype=jnp.int32)
    host_of = flat // replicas
    local = flat % replicas
    copy = jnp.clip(local - exp_host, 0, rep_host - 1)
    copied = ((host_of - 1 - copy) % groups) * exp_host + plan_layer[host_of, copy]
    return jnp.where(local < exp_host, host_of * exp_host + local, copied)


def kept_slots(experts, picks, table, capacity):
    flat_e = experts.reshape(-1)
    matches = (table[None, :] == flat_e[:, None]).astype(jnp.int32)
    rank = jnp.cumsum(matches, axis=1) - 1
    wanted = picks.reshape(-1) % jnp.sum(matches, axis=1)
    chosen = matches * (rank == wanted[:, None]).astype(jnp.int32)
    before = jnp.cumsum(chosen, axis=0) - chosen
    return (jnp.sum(before * chosen, axis=1) < capacity).reshape(experts.shape)


def plain_device(tokens, norm_gain, gate_weight, up_weight, down_weight, replica_plan, route_expert, replica_pick, combine_num):
    groups = lax.axis_size("dp")
    host = lax.axis_index("dp")
    layers, _ = norm_gain.shape
    exp_host = gate_weight.shape[1]
    rep_host = replica_plan.shape[2]
    rows, _ = tokens.shape
    count = groups * rows
    top = route_expert.shape[2]
    stream = lax.all_gather(tokens, "dp", axis=0, tiled=True)
    numbers = lax.all_gather(combine_num, "dp", axis=1, tiled=True).astype(f32)
    own_ids = host * exp_host + jnp.arange(exp_host, dtype=jnp.int32)
    for layer in range(layers):
        table = serve_table(replica_plan[layer], groups, exp_host, rep_host)
        kept = jax.vmap(lambda e, p: kept_slots(e, p, table, rows // 2))(
            route_expert[layer].reshape(groups, rows, top), replica_pick[layer].reshape(groups, rows, top)
        ).reshape(count, top)
        weights = numbers[layer] / jnp.sum(numbers[layer], axis=1, keepdims=True) * kept
        hits = route_expert[layer][:, :, None] == own_ids[None, None, :]
        combine = jnp.sum(weights[:, :, None] * hits, axis=1)
        whole = lax.all_gather(stream, "ep", axis=1, tiled=True).astype(f32)
        inverse = lax.rsqrt(jnp.mean(whole * whole, axis=1, keepdims=True) + epsilon)
        normed = (whole * inverse * norm_gain[layer][None, :]).astype(bf16)
        gate = jnp.einsum("nd,rfd->rnf", normed, gate_weight[layer], preferred_element_type=f32)
        up = jnp.einsum("nd,rfd->rnf", normed, up_weight[layer], preferred_element_type=f32)
        hidden = (jax.nn.silu(gate) * up * combine.T[:, :, None]).astype(bf16)
        hidden = lax.all_gather(hidden, "ep", axis=2, tiled=True)
        partial = jnp.einsum("rnf,rdf->nd", hidden, down_weight[layer], preferred_element_type=f32)
        parts = lax.all_gather(partial.astype(bf16), "dp", axis=0).astype(f32)
        update = jnp.sum(parts, axis=0)
        stream = (stream.astype(f32) + update).astype(bf16)
    stream = lax.dynamic_slice_in_dim(stream, host * rows, rows, 0)
    update = lax.dynamic_slice_in_dim(update, host * rows, rows, 0)
    return stream, update.astype(bf16)


def per_device(*args):
    tokens, norm_gain, gate_weight = args[:3]
    groups, shards = lax.axis_size("dp"), lax.axis_size("ep")
    layers, units = norm_gain.shape[0], gate_weight.shape[2]
    rows, width = tokens.shape
    fits = (
        groups & (groups - 1) == 0
        and shards & (shards - 1) == 0
        and 4 <= shards <= widest
        and width % lanes == 0
        and units % lanes == 0
        and rows % 16 == 0
        and groups * rows <= lanes
        and layers * args[6].shape[2] <= rows
        and args[6].shape[2] % 8 == 0
    )
    return fast_device(*args) if fits else plain_device(*args)


def solution(mesh):
    return jax.shard_map(
        per_device,
        mesh=mesh,
        in_specs=(
            P("dp", "ep"),
            P(),
            P(None, "dp", "ep", None),
            P(None, "dp", "ep", None),
            P(None, "dp", "ep", None),
            P(),
            P(),
            P(),
            P(None, "dp", None),
        ),
        out_specs=(P("dp", "ep"), P("dp", "ep")),
        check_vma=False,
    )
```

```python
import functools

import jax
import jax.numpy as jnp
from jax import lax
from jax.experimental import pallas as pl
from jax.experimental.pallas import tpu as pltpu
from jax.sharding import PartitionSpec as P


epsilon = 1e-06
lanes = 128
widest = 8
bf16 = jnp.bfloat16
f32 = jnp.float32


def routing(plan_ref, route_ref, pick_ref, mask_ref, sizes):
    layers, groups, rows, top, exp_host, rep_host, capacity = sizes
    host = lax.axis_index("dp")
    replicas = exp_host + rep_host
    tokens = groups * rows
    slots = -(-groups * replicas // 8) * 8
    slot_i = lax.broadcasted_iota(jnp.int32, (slots, 1), 0)
    from_i = lax.broadcasted_iota(jnp.int32, (tokens, lanes), 0)
    to_i = lax.broadcasted_iota(jnp.int32, (tokens, lanes), 1)
    earlier = jnp.where((from_i // rows == to_i // rows) & (from_i < to_i), 1.0, 0.0).astype(bf16)[:, :tokens]
    swap = jnp.where((from_i // rows == (to_i // rows) ^ host) & (from_i % rows == to_i % rows), 1.0, 0.0).astype(bf16)
    for layer in range(layers):
        served = []
        for slot in range(groups * replicas):
            owner, local = divmod(slot, replicas)
            if local < exp_host:
                served.append(owner * exp_host + local)
            else:
                copy = local - exp_host
                served.append(((owner - 1 - copy) % groups) * exp_host + plan_ref[layer, copy, owner])
        table = jnp.full((slots, 1), -1, jnp.int32)
        for slot, expert in enumerate(served):
            table = jnp.where(slot_i == slot, expert, table)
        rank = jnp.zeros((slots, 1), f32)
        count = jnp.zeros((slots, 1), f32)
        for slot, expert in enumerate(served):
            same = jnp.where(table == expert, 1.0, 0.0)
            count = count + same
            rank = rank + jnp.where(slot_i > slot, same, 0.0)
        count = jnp.broadcast_to(jnp.maximum(count, 1.0), (slots, tokens))
        rank = jnp.broadcast_to(rank, (slots, tokens))
        table = jnp.broadcast_to(table, (slots, tokens))
        experts = route_ref[layer]
        picks = pick_ref[layer].astype(f32)
        chosen = []
        for k in range(top):
            pick = picks[k : k + 1, :]
            wanted = pick - count * jnp.floor((pick + 0.5) / count)
            chosen.append(jnp.where((experts[k : k + 1, :] == table) & (rank == wanted), 1.0, 0.0))
        total = functools.reduce(lambda a, b: a + b, chosen)
        before = jnp.dot(total.astype(bf16), earlier, preferred_element_type=f32)
        kept = []
        for k in range(top):
            position = jnp.sum(before * chosen[k], axis=0, keepdims=True)
            before = before + chosen[k]
            kept.append(jnp.where(position < capacity - 0.5, 1.0, 0.0))
        kept = jnp.concatenate(kept, axis=0)
        for j in range(exp_host):
            mask = jnp.where(experts == host * exp_host + j, kept, 0.0)
            mask_ref[layer, j] = jnp.dot(mask.astype(bf16), swap, preferred_element_type=f32)


def slabs(source, target, ks, size, sems):
    column = lax.axis_index("ep")
    moves = []
    for i, k in enumerate(ks):
        block = pl.ds(pl.multiple_of((column ^ k) * size, lanes), size)
        moves.append(pltpu.make_async_copy(source.at[:, :, block], target.at[:, :, block], sems.at[i]))
    return moves


def setup_kernel(
    x_ref, ups_ref, plan_hbm, route_hbm, pick_hbm, gain_hbm, weight_hbm, mask_ref, gain_ref, weight_ref, sums_ref, total_ref,
    plan_ref, route_ref, pick_ref, sems, slab_sems, *, sizes, shards, units, width,
):
    small = [(plan_hbm, plan_ref), (route_hbm, route_ref), (pick_hbm, pick_ref)]
    small.append((gain_hbm, gain_ref.at[:, pl.ds(0, gain_hbm.shape[1])]))
    moves = [pltpu.make_async_copy(src, dst, sems.at[i]) for i, (src, dst) in enumerate(small)]
    heavy = slabs(weight_hbm.at[0], weight_ref, range(shards), width, slab_sems)
    for move in moves + heavy:
        move.start()
    for move in moves[:3]:
        move.wait()
    routing(plan_ref, route_ref, pick_ref, mask_ref, sizes)
    moves[3].wait()
    heavy[0].wait()
    squares, sums = feature_sums((weight_ref, ups_ref), gain_ref, [x_ref], (0,), 0, sizes[4], units, width)
    tokens = x_ref.shape[0]
    for i, part in enumerate(sums):
        sums_ref[i, :, :tokens] = part
    total_ref[...] = jnp.broadcast_to(squares, (tokens, lanes))
    for move in heavy[1:]:
        move.wait()


def early_kernel(_, weight_hbm, result_ref, sems, *, ks, width):
    moves = slabs(weight_hbm.at[0], result_ref, ks, width, sems)
    for move in moves:
        move.start()
    for move in moves:
        move.wait()


def early(after, weight, ks, width):
    return pl.pallas_call(
        functools.partial(early_kernel, ks=ks, width=width),
        out_shape=pltpu.VMEM(weight.shape[1:], weight.dtype),
        in_specs=[any_spec(), hbm_spec()],
        out_specs=vmem_spec(),
        scratch_shapes=[pltpu.SemaphoreType.DMA((len(ks),))],
        compiler_params=pltpu.CompilerParams(vmem_limit_bytes=2**20),
        cost_estimate=pl.CostEstimate(flops=4 * 10**9, bytes_accessed=2 * 10**7, transcendentals=0),
        name="early",
    )(after, in_hbm(weight))


def prefetch_kernel(*refs, layer, count):
    sources, results, sems = refs[-2 * count - 1 : -count - 1], refs[-count - 1 : -1], refs[-1]
    moves = [
        pltpu.make_async_copy(src.at[layer], dst, sems.at[i]) for i, (src, dst) in enumerate(zip(sources, results))
    ]
    for move in moves:
        move.start()
    for move in moves:
        move.wait()


def feature_sums(weight_refs, gain_ref, x_refs, ks, layer, exp_host, units, width):
    column = lax.axis_index("ep")
    offsets = [pl.multiple_of((column ^ k) * width, lanes) for k in ks]
    squares, scaled = 0.0, []
    for x_ref, offset in zip(x_refs, offsets):
        x = x_ref[...].astype(f32)
        squares = squares + jnp.sum(x * x, axis=1, keepdims=True)
        scaled.append((x * gain_ref[layer : layer + 1, pl.ds(offset, width)]).astype(bf16))
    scaled = jnp.concatenate(scaled, axis=1)
    sums = []
    for weight_ref in weight_refs:
        weight = jnp.concatenate([weight_ref[:, :, pl.ds(offset, width)] for offset in offsets], axis=2)
        weight = weight.reshape(exp_host * units, len(ks) * width)
        sums.append(lax.dot_general(weight, scaled, (((1,), (1,)), ((), ())), preferred_element_type=f32))
    return squares, sums


def gate_part(*refs, layer, ks, first, last, fill, top, rows, shards, exp_host, units, width):
    refs = list(refs)
    gate_ref, up_ref, gain_ref = refs[:3]
    x_refs = refs[3 : 3 + len(ks)]
    refs = refs[3 + len(ks) :]
    moves = []
    if not first:
        sums_ref, squares_ref = refs[:2]
        refs = refs[2:]
    if fill:
        source = refs.pop(0)
        sems = refs.pop()
        up_ref = refs.pop()
        moves = slabs(source.at[layer], up_ref, fill, width, sems)
        for move in moves:
            move.start()
    if last:
        mask_ref, num_ref, out_ref, acc_ref = refs
    else:
        acc_ref, total_ref = refs
    tokens = x_refs[0].shape[0]
    squares, sums = feature_sums((gate_ref, up_ref), gain_ref, x_refs, ks, layer, exp_host, units, width)
    if not first:
        squares = squares + squares_ref[:, 0:1]
    for i, part in enumerate(sums):
        acc_ref[i, :, :tokens] = part if first else sums_ref[i, :, :tokens] + part
    for move in moves:
        move.wait()
    if not last:
        total_ref[...] = jnp.broadcast_to(squares, (tokens, lanes))
        return
    inverse = lax.rsqrt(squares / (shards * width) + epsilon)
    turned = jnp.concatenate([jnp.broadcast_to(inverse, (tokens, lanes)), jnp.zeros((lanes - tokens, lanes), f32)], axis=0).T
    scale = turned[0:1, :]
    numbers = num_ref[0:rows, :].astype(f32)
    for b in range(1, num_ref.shape[0] // rows):
        numbers = numbers + pltpu.roll(num_ref[b * rows : (b + 1) * rows, :].astype(f32), b * rows, 1)
    numbers = numbers[layer * top : (layer + 1) * top, :]
    shares = numbers / jnp.maximum(jnp.sum(numbers, axis=0, keepdims=True), 1.0)
    for j in range(exp_host):
        weight = jnp.sum(mask_ref[layer, j] * shares, axis=0, keepdims=True)
        gate = acc_ref[0, j * units : (j + 1) * units, :] * scale
        up = acc_ref[1, j * units : (j + 1) * units, :] * scale
        hidden = gate / (1.0 + jnp.exp(-gate)) * up * weight
        out_ref[j * tokens : (j + 1) * tokens, :] = hidden.T[:tokens].astype(bf16)


def gate_up(layer, ks, gates, ups, gains, xs, sums, finish, sizes, units, width, shards, load=None, fill=()):
    _, groups, rows, top, exp_host, _, _ = sizes
    count = groups * rows
    sums_shape = pltpu.VMEM((2, exp_host * units, lanes), f32)
    last = finish is not None
    operands = [gates, ups, gains] + [xs[k] for k in ks] + list(sums or ()) + list(finish or ())
    in_specs = [vmem_spec()] * len(operands)
    out_shape = [pltpu.VMEM((exp_host * count, units), bf16)] if last else [sums_shape, pltpu.VMEM((count, lanes), f32)]
    scratch = [sums_shape] if last else []
    aliases = {}
    if load is not None:
        operands.append(in_hbm(load))
        in_specs.append(hbm_spec())
        out_shape.append(pltpu.VMEM(load.shape[1:], load.dtype))
        scratch.append(pltpu.SemaphoreType.DMA((len(fill),)))
        aliases = {1: len(out_shape) - 1}
    work = 2 * 2 * exp_host * units * width * len(ks) * count
    return pl.pallas_call(
        functools.partial(
            gate_part,
            layer=layer,
            ks=ks,
            first=sums is None,
            last=last,
            fill=fill,
            top=top,
            rows=rows,
            shards=shards,
            exp_host=exp_host,
            units=units,
            width=width,
        ),
        out_shape=out_shape,
        in_specs=in_specs,
        out_specs=[vmem_spec()] * len(out_shape),
        scratch_shapes=scratch,
        input_output_aliases=aliases,
        compiler_params=pltpu.CompilerParams(vmem_limit_bytes=8 * 2**20),
        cost_estimate=pl.CostEstimate(flops=work, bytes_accessed=work // count, transcendentals=0),
    )(*operands)


def down_part(*refs, ks, first, last, exp_host, units, tokens):
    down_ref = refs[0]
    h_refs = refs[1 : 1 + len(ks)]
    refs = refs[1 + len(ks) :]
    column = lax.axis_index("ep")
    parts, weights = [], []
    for h_ref, k in zip(h_refs, ks):
        offset = pl.multiple_of((column ^ k) * units, lanes)
        for j in range(exp_host):
            parts.append(h_ref[j * tokens : (j + 1) * tokens, :])
            weights.append(down_ref[j, :, pl.ds(offset, units)])
    part = lax.dot_general(
        jnp.concatenate(weights, axis=1),
        jnp.concatenate(parts, axis=1),
        (((1,), (1,)), ((), ())),
        preferred_element_type=f32,
    )
    if not first:
        part = refs[0][:, :tokens] + part
        refs = refs[1:]
    if not last:
        refs[0][:, :tokens] = part
        return
    own_ref, send_ref, acc_ref = refs
    acc_ref[:, :tokens] = part
    result = acc_ref[...].T[:tokens]
    own_ref[...] = result
    send_ref[...] = result.astype(bf16)


def down_first_kernel(h_ref, weight_hbm, weight_ref, sums_ref, sems, *, layer, shards, exp_host, units, tokens):
    moves = slabs(weight_hbm.at[layer], weight_ref, range(shards), units, sems)
    for move in moves:
        move.start()
    moves[0].wait()
    down_part(weight_ref, h_ref, sums_ref, ks=(0,), first=True, last=False, exp_host=exp_host, units=units, tokens=tokens)
    for move in moves[1:]:
        move.wait()


def down_first(layer, weight, hidden, shards, count, units, width, exp_host):
    return pl.pallas_call(
        functools.partial(
            down_first_kernel, layer=layer, shards=shards, exp_host=exp_host, units=units, tokens=count
        ),
        out_shape=[pltpu.VMEM(weight.shape[1:], weight.dtype), pltpu.VMEM((width, lanes), f32)],
        in_specs=[vmem_spec(), hbm_spec()],
        out_specs=[vmem_spec()] * 2,
        scratch_shapes=[pltpu.SemaphoreType.DMA((shards,))],
        compiler_params=pltpu.CompilerParams(vmem_limit_bytes=8 * 2**20),
        cost_estimate=pl.CostEstimate(flops=4 * 10**9, bytes_accessed=2 * 10**7, transcendentals=0),
    )(hidden, in_hbm(weight))


def down(ks, downs, hs, sums, last, count, units, width, exp_host):
    sums_shape = pltpu.VMEM((width, lanes), f32)
    operands = [downs] + [hs[k] for k in ks] + ([] if sums is None else [sums])
    work = 2 * exp_host * units * width * len(ks) * count
    return pl.pallas_call(
        functools.partial(
            down_part, ks=ks, first=sums is None, last=last, exp_host=exp_host, units=units, tokens=count
        ),
        out_shape=(pltpu.VMEM((count, width), f32), pltpu.VMEM((count, width), bf16)) if last else sums_shape,
        in_specs=[vmem_spec()] * len(operands),
        out_specs=(vmem_spec(), vmem_spec()) if last else vmem_spec(),
        scratch_shapes=[sums_shape] if last else [],
        compiler_params=pltpu.CompilerParams(vmem_limit_bytes=8 * 2**20),
        cost_estimate=pl.CostEstimate(flops=work, bytes_accessed=work // count, transcendentals=0),
    )(*operands)


def pack_kernel(tokens_hbm, numbers_hbm, out_ref, numbers_ref, sems, *, width):
    moves = [
        pltpu.make_async_copy(numbers_hbm, numbers_ref, sems.at[0]),
        pltpu.make_async_copy(tokens_hbm, out_ref.at[:, pl.ds(0, width)], sems.at[1]),
    ]
    for move in moves:
        move.start()
    layers, top, rows = numbers_ref.shape
    out_ref[:, width:] = jnp.zeros((out_ref.shape[0], lanes), bf16)
    moves[0].wait()
    numbers = jnp.concatenate([numbers_ref[layer] for layer in range(layers)], axis=0)
    out_ref[: layers * top, width : width + rows] = numbers.astype(f32).astype(bf16)
    moves[1].wait()


def pack(tokens, combine_num):
    rows, width = tokens.shape
    layers, _, top = combine_num.shape
    return pl.pallas_call(
        functools.partial(pack_kernel, width=width),
        out_shape=pltpu.VMEM((rows, width + lanes), bf16),
        in_specs=[hbm_spec()] * 2,
        out_specs=vmem_spec(),
        scratch_shapes=[pltpu.VMEM((layers, top, rows), jnp.int32), pltpu.SemaphoreType.DMA((2,))],
        compiler_params=pltpu.CompilerParams(vmem_limit_bytes=2**20),
        name="pack",
    )(in_hbm(tokens), in_hbm(combine_num.transpose(0, 2, 1)))


def vmem_spec():
    return pl.BlockSpec(memory_space=pltpu.VMEM)


def hbm_spec():
    return pl.BlockSpec(memory_space=pltpu.HBM)


def any_spec():
    return pl.BlockSpec(memory_space=pl.ANY)


def in_hbm(value):
    return pltpu.with_memory_space_constraint(value, pltpu.HBM)


def prefetch(layer, after, *weights):
    size = sum(w.size // w.shape[0] * w.dtype.itemsize for w in weights)
    return pl.pallas_call(
        functools.partial(prefetch_kernel, layer=layer, count=len(weights)),
        out_shape=tuple(pltpu.VMEM(w.shape[1:], w.dtype) for w in weights),
        in_specs=[any_spec()] + [hbm_spec()] * len(weights),
        out_specs=tuple(vmem_spec() for _ in weights),
        scratch_shapes=[pltpu.SemaphoreType.DMA((len(weights),))],
        compiler_params=pltpu.CompilerParams(vmem_limit_bytes=2**20),
        cost_estimate=pl.CostEstimate(flops=400 * size, bytes_accessed=2 * size, transcendentals=0),
    )(after, *[in_hbm(w) for w in weights])


def xor_permute(value, axis, size, bits):
    return lax.ppermute(value, axis, [(i, i ^ bits) for i in range(size)])


def gather_shards(value, size):
    same = {0: value}
    for k in sorted(range(2, size, 2), reverse=True):
        same[k] = xor_permute(value, "ep", size, k)
    both = {}
    for k, part in same.items():
        both[k] = part
        both[k + 1] = xor_permute(part, "ep", size, 1)
    return [both[k] for k in range(size)]


def fast_device(tokens, norm_gain, gate_weight, up_weight, down_weight, replica_plan, route_expert, replica_pick, combine_num):
    groups = lax.axis_size("dp")
    shards = lax.axis_size("ep")
    layers = norm_gain.shape[0]
    exp_host, units = gate_weight.shape[1:3]
    rep_host = replica_plan.shape[2]
    rows, width = tokens.shape
    count = groups * rows
    top = route_expert.shape[2]
    capacity = rows // 2
    sizes = (layers, groups, rows, top, exp_host, rep_host, capacity)

    same = tuple(range(0, shards, 2))
    late = tuple(k + 1 for k in same)
    payload = pack(tokens, combine_num)
    gathered = [payload]
    ups = early(payload, up_weight, same + late[:2], width)
    for k in range(1, groups):
        gathered.append(xor_permute(payload, "dp", groups, k))
    gathered = jnp.concatenate(gathered, axis=0)
    stream = gathered[:, :width]
    number = gathered[:, width:]

    prepare = pl.pallas_call(
        functools.partial(setup_kernel, sizes=sizes, shards=shards, units=units, width=width),
        out_shape=(
            pltpu.VMEM((layers, exp_host, top, lanes), f32),
            pltpu.VMEM((layers, norm_gain.shape[1] + 4 * lanes), f32),
            pltpu.VMEM(gate_weight.shape[1:], bf16),
            pltpu.VMEM((2, exp_host * units, lanes), f32),
            pltpu.VMEM((count, lanes), f32),
        ),
        in_specs=[vmem_spec()] * 2 + [hbm_spec()] * 5,
        out_specs=(vmem_spec(),) * 5,
        scratch_shapes=[
            pltpu.SMEM((layers, rep_host, groups), jnp.int32),
            pltpu.VMEM((layers, top, count), jnp.int32),
            pltpu.VMEM((layers, top, count), jnp.int32),
            pltpu.SemaphoreType.DMA((4,)),
            pltpu.SemaphoreType.DMA((shards,)),
        ],
        compiler_params=pltpu.CompilerParams(vmem_limit_bytes=8 * 2**20),
        cost_estimate=pl.CostEstimate(flops=4 * 10**9, bytes_accessed=2 * 10**7, transcendentals=0),
        name="setup",
    )
    small = (replica_plan, route_expert, replica_pick)
    small = [in_hbm(v.transpose(0, 2, 1)) for v in small] + [in_hbm(norm_gain), in_hbm(gate_weight)]
    mask, gains, gates, *sums = prepare(stream, ups, *small)

    for layer in range(layers):
        xs = gather_shards(stream, shards)
        dims = (sizes, units, width, shards)
        finish = (mask, number)
        if layer == 0:
            *sums, ups = gate_up(
                layer, same[1:], gates, ups, gains, xs, sums, None, *dims, load=up_weight, fill=late[2:]
            )
            (hidden,) = gate_up(layer, late, gates, ups, gains, xs, sums, finish, *dims)
        else:
            sums = gate_up(layer, (0, 1), gates, ups, gains, xs, None, None, *dims)
            sums = gate_up(layer, same[1:], gates, ups, gains, xs, sums, None, *dims)
            (hidden,) = gate_up(layer, late[1:], gates, ups, gains, xs, sums, finish, *dims)
        hs = gather_shards(hidden, shards)
        dims = (count, units, width, exp_host)
        downs, sums = down_first(layer, down_weight, hidden, shards, *dims)
        sums = down(same[1:], downs, hs, sums, False, *dims)
        own, send = down(late, downs, hs, sums, True, *dims)
        if layer + 1 < layers:
            gates, ups = prefetch(layer + 1, send, gate_weight, up_weight)
            update = own
            for k in range(1, groups):
                other = xor_permute(send, "dp", groups, k).astype(f32)
                blocks = [other[(b ^ k) * rows : ((b ^ k) + 1) * rows] for b in range(groups)]
                update = update + jnp.concatenate(blocks, axis=0)
        else:
            update = own[:rows]
            for k in range(1, groups):
                other = xor_permute(send[k * rows : (k + 1) * rows], "dp", groups, k)
                update = update + other.astype(f32)
            stream = stream[:rows]
        stream = (stream.astype(f32) + update).astype(bf16)
    return stream, update.astype(bf16)


def serve_table(plan_layer, groups, exp_host, rep_host):
    replicas = exp_host + rep_host
    flat = jnp.arange(groups * replicas, dtype=jnp.int32)
    host_of = flat // replicas
    local = flat % replicas
    copy = jnp.clip(local - exp_host, 0, rep_host - 1)
    copied = ((host_of - 1 - copy) % groups) * exp_host + plan_layer[host_of, copy]
    return jnp.where(local < exp_host, host_of * exp_host + local, copied)


def kept_slots(experts, picks, table, capacity):
    flat_e = experts.reshape(-1)
    matches = (table[None, :] == flat_e[:, None]).astype(jnp.int32)
    rank = jnp.cumsum(matches, axis=1) - 1
    wanted = picks.reshape(-1) % jnp.sum(matches, axis=1)
    chosen = matches * (rank == wanted[:, None]).astype(jnp.int32)
    before = jnp.cumsum(chosen, axis=0) - chosen
    return (jnp.sum(before * chosen, axis=1) < capacity).reshape(experts.shape)


def plain_device(tokens, norm_gain, gate_weight, up_weight, down_weight, replica_plan, route_expert, replica_pick, combine_num):
    groups = lax.axis_size("dp")
    host = lax.axis_index("dp")
    layers, _ = norm_gain.shape
    exp_host = gate_weight.shape[1]
    rep_host = replica_plan.shape[2]
    rows, _ = tokens.shape
    count = groups * rows
    top = route_expert.shape[2]
    stream = lax.all_gather(tokens, "dp", axis=0, tiled=True)
    numbers = lax.all_gather(combine_num, "dp", axis=1, tiled=True).astype(f32)
    own_ids = host * exp_host + jnp.arange(exp_host, dtype=jnp.int32)
    for layer in range(layers):
        table = serve_table(replica_plan[layer], groups, exp_host, rep_host)
        kept = jax.vmap(lambda e, p: kept_slots(e, p, table, rows // 2))(
            route_expert[layer].reshape(groups, rows, top), replica_pick[layer].reshape(groups, rows, top)
        ).reshape(count, top)
        weights = numbers[layer] / jnp.sum(numbers[layer], axis=1, keepdims=True) * kept
        hits = route_expert[layer][:, :, None] == own_ids[None, None, :]
        combine = jnp.sum(weights[:, :, None] * hits, axis=1)
        whole = lax.all_gather(stream, "ep", axis=1, tiled=True).astype(f32)
        inverse = lax.rsqrt(jnp.mean(whole * whole, axis=1, keepdims=True) + epsilon)
        normed = (whole * inverse * norm_gain[layer][None, :]).astype(bf16)
        gate = jnp.einsum("nd,rfd->rnf", normed, gate_weight[layer], preferred_element_type=f32)
        up = jnp.einsum("nd,rfd->rnf", normed, up_weight[layer], preferred_element_type=f32)
        hidden = (jax.nn.silu(gate) * up * combine.T[:, :, None]).astype(bf16)
        hidden = lax.all_gather(hidden, "ep", axis=2, tiled=True)
        partial = jnp.einsum("rnf,rdf->nd", hidden, down_weight[layer], preferred_element_type=f32)
        parts = lax.all_gather(partial.astype(bf16), "dp", axis=0).astype(f32)
        update = jnp.sum(parts, axis=0)
        stream = (stream.astype(f32) + update).astype(bf16)
    stream = lax.dynamic_slice_in_dim(stream, host * rows, rows, 0)
    update = lax.dynamic_slice_in_dim(update, host * rows, rows, 0)
    return stream, update.astype(bf16)


def per_device(*args):
    tokens, norm_gain, gate_weight = args[:3]
    groups, shards = lax.axis_size("dp"), lax.axis_size("ep")
    layers, units = norm_gain.shape[0], gate_weight.shape[2]
    rows, width = tokens.shape
    fits = (
        groups & (groups - 1) == 0
        and shards & (shards - 1) == 0
        and shards == widest
        and width % lanes == 0
        and units % lanes == 0
        and rows % 16 == 0
        and groups * rows <= lanes
        and layers * args[6].shape[2] <= rows
        and args[6].shape[2] % 8 == 0
    )
    return fast_device(*args) if fits else plain_device(*args)


def solution(mesh):
    return jax.shard_map(
        per_device,
        mesh=mesh,
        in_specs=(
            P("dp", "ep"),
            P(),
            P(None, "dp", "ep", None),
            P(None, "dp", "ep", None),
            P(None, "dp", "ep", None),
            P(),
            P(),
            P(),
            P(None, "dp", None),
        ),
        out_specs=(P("dp", "ep"), P("dp", "ep")),
        check_vma=False,
    )
```
